128 devices in a mesh: node: 128 (over x, z, y, core).
Axes of the slice: x: 4, y: 4, z: 4, core: 2. Of those that a mesh axis runs over, the one named last changes fastest.
Arguments:
- event_node: int32 [65536], P('node'), may hold values from 0 to 32767, as said below
- neighbours: int32 [65536, 10], P('node'), may hold values from 0 to 32767, as said below
- event_bucket: int32 [65536], P('node'), may hold values from 0 to 127
- neighbour_bucket: int32 [65536, 10], P('node'), may hold values from 0 to 127
- edge_features: bfloat16 [65536, 128], P('node'), may hold values from -6 to 6
- affinity: float32 [65536, 10], P('node'), may hold values from -320 to 320
- upstream: bfloat16 [65536, 512], P('node'), may hold values from -6 to 6
- node_memory: bfloat16 [32768, 512], P('node'), may hold values from -4 to 4
- edge_weight: bfloat16 [128, 512], replicated, may hold values from -0.5 to 0.5
- time_message: float32 [128, 512], replicated, may hold values from -6 to 6
- input_weight: bfloat16 [512, 1536], replicated, may hold values from -0.25 to 0.25
- hidden_weight: bfloat16 [512, 1536], replicated, may hold values from -0.25 to 0.25
- gate_bias: float32 [1536], replicated, may hold values from -6 to 6
- time_key: float32 [128, 512], replicated, may hold values from -6 to 6
- query_weight: bfloat16 [512, 512], replicated, may hold values from -0.25 to 0.25
- key_weight: bfloat16 [512, 512], replicated, may hold values from -0.25 to 0.25
- value_weight: bfloat16 [512, 512], replicated, may hold values from -0.25 to 0.25
- out_weight: bfloat16 [512, 512], replicated, may hold values from -0.25 to 0.25
Outputs:
- embedding: bfloat16 [65536, 512], P('node')
- new_memory: bfloat16 [32768, 512], P('node')
- grad_query: float32 [512, 512], replicated
- grad_key: float32 [512, 512], replicated
- grad_value: float32 [512, 512], replicated
- grad_out: float32 [512, 512], replicated
The draws below stay inside these ranges and needn't reach their ends.
Inputs may be any that keep to these rules, and one draw needn't show every extreme that they name: `event_node`: node i belongs to index i // 256 of node. Of the 512 rows of one device, at most 12 name nodes of one index; in every draw one index receives exactly 12 of them from every device. `neighbours`: node i belongs to index i // 256 of node. Of the 5120 entries of one device's rows, at most 80 name nodes of one index, and these name at most 64 distinct nodes; in every draw one index receives exactly 80 entries naming exactly 64 distinct nodes from every device.
All inputs are finite; a program needn't handle non-finite values.
Results may differ from the reference program's by a relative error of at most 0.012.
Values may be sent and summed in bfloat16 or wider, within the bound.
No kernel may reach another device: no remote copies, remote signals or barrier semaphores. Data moves between devices by JAX's collectives and lax.ppermute only.
A program may use at most 192 MiB of HBM per device.

```python
import math
import jax
import jax.numpy as jnp
from jax import lax

MEM = 512
MSG = 512
EDGE = 128
HEADS = 2
NEIGH = 10
TBUCK = 128
CAPU = 64
EV_DEV = 512
NODE_DEV = 256
EVENTS = 65536
NODES = 32768
CAPM = 12
CAPN = 80
N_NODE = 128


def packed_owners(device_key, amount, capacity, hottest):
    slots_all = N_NODE * capacity
    slot_ids = jnp.arange(slots_all, dtype=jnp.int32)
    owners = slot_ids // capacity
    within = slot_ids % capacity
    priority = jax.random.permutation(jax.random.fold_in(device_key, 1), slots_all).astype(jnp.int32) + 1
    priority = jnp.where(owners == hottest, 0, priority)
    ordered = jnp.argsort(priority, stable=True)[:amount]
    shuffled = ordered[jax.random.permutation(jax.random.fold_in(device_key, 2), amount)]
    return (owners[shuffled], within[shuffled])


def draw_event_node(key, part):
    hottest = jax.random.randint(jax.random.fold_in(key, 11), (), 0, N_NODE)

    def device(number):
        device_key = jax.random.fold_in(jax.random.fold_in(key, 12), number)
        owners, within = packed_owners(device_key, EV_DEV, CAPM, hottest)
        local_rows = jax.random.randint(jax.random.fold_in(device_key, 3), (EV_DEV,), 0, NODE_DEV)
        return owners * NODE_DEV + local_rows
    return jax.vmap(device)(jnp.arange(N_NODE, dtype=jnp.int32)).reshape(-1).astype(jnp.int32)


def draw_neighbours(key, part):
    hottest = jax.random.randint(jax.random.fold_in(key, 21), (), 0, N_NODE)

    def device(number):
        device_key = jax.random.fold_in(jax.random.fold_in(key, 22), number)
        owners, within = packed_owners(device_key, EV_DEV * NEIGH, CAPN, hottest)

        def pool_of(owner_id):
            return jax.random.permutation(jax.random.fold_in(device_key, 1000 + owner_id), NODE_DEV)[:CAPU]
        pools = jax.vmap(pool_of)(jnp.arange(N_NODE, dtype=jnp.int32))
        local_rows = pools[owners, within % CAPU]
        return (owners * NODE_DEV + local_rows).reshape(EV_DEV, NEIGH)
    whole = jax.vmap(device)(jnp.arange(N_NODE, dtype=jnp.int32))
    return whole.reshape(EV_DEV * N_NODE, NEIGH).astype(jnp.int32)


def draw_affinity(key, part):
    rows_all = EV_DEV * N_NODE
    return jax.random.normal(jax.random.fold_in(key, 1), (rows_all, NEIGH), jnp.float32)


def touch_ends(entries, stream_key, smallest, high):
    spot = [jax.random.randint(jax.random.fold_in(stream_key, axis), (), 0, length) for axis, length in enumerate(entries.shape)]
    longest = entries.shape.index(max(entries.shape))
    beside = spot[:longest] + [(spot[longest] + 1) % entries.shape[longest]] + spot[longest + 1:]
    return entries.at[tuple(spot)].set(smallest).at[tuple(beside)].set(high)


def block_scale(rng, shape, split, least, high):
    level, own = 1.0, jax.random.fold_in(rng, 6)
    for dim, shards_of in split:
        draws = jnp.exp(jax.random.uniform(jax.random.fold_in(own, dim), (shards_of,), jnp.float32, least / len(split), high / len(split)))
        level = level * jnp.repeat(draws, shape[dim] // shards_of).reshape([-1 if axis == dim else 1 for axis in range(len(shape))])
    return level


def scatter_about(rng, extent, width, reach, shards=(), kind=jnp.bfloat16):
    drawn = jax.random.normal(rng, extent, jnp.float32) * width
    if len(shards) > 0:
        drawn = block_scale(rng, extent, shards, -0.22, 0.18) * drawn
    return jnp.clip(drawn, min=-reach, max=reach).astype(kind)


def setup_inputs(seed: int = 0) -> dict:
    seeds = jax.random.split(jax.random.key(seed), 19)
    event_node = draw_event_node(jax.random.fold_in(seeds[18], 71), 0)
    neighbours = draw_neighbours(jax.random.fold_in(seeds[18], 71), 0)
    event_bucket = touch_ends(jax.random.randint(seeds[2], (EVENTS,), 0, TBUCK), jax.random.fold_in(seeds[2], 1), 0, TBUCK - 1).astype(jnp.int32)
    neighbour_bucket = touch_ends(jax.random.randint(seeds[3], (EVENTS, NEIGH), 0, TBUCK), jax.random.fold_in(seeds[3], 1), 0, TBUCK - 1).astype(jnp.int32)
    edge_features = scatter_about(seeds[4], (EVENTS, EDGE), 1.0, 6.0, ((0, 128),))
    affinity = draw_affinity(jax.random.fold_in(seeds[18], 71), 0)
    upstream = scatter_about(seeds[6], (EVENTS, MEM), 1.0, 6.0, ((0, 128),))
    node_memory = scatter_about(seeds[7], (NODES, MEM), 1.0, 4.0, ((0, 128),))
    edge_weight = scatter_about(seeds[8], (EDGE, MSG), EDGE ** -0.5, 0.5)
    time_message = scatter_about(seeds[9], (TBUCK, MSG), 1.0, 6.0, (), jnp.float32)
    input_weight = scatter_about(seeds[10], (MSG, 3 * MEM), MSG ** -0.5, 0.25)
    hidden_weight = scatter_about(seeds[11], (MEM, 3 * MEM), MEM ** -0.5, 0.25)
    gate_bias = scatter_about(seeds[12], (3 * MEM,), 1.0, 6.0, (), jnp.float32)
    time_key = scatter_about(seeds[13], (TBUCK, MEM), 1.0, 6.0, (), jnp.float32)
    query_weight = scatter_about(seeds[14], (MEM, MEM), MEM ** -0.5, 0.25)
    key_weight = scatter_about(seeds[15], (MEM, MEM), MEM ** -0.5, 0.25)
    value_weight = scatter_about(seeds[16], (MEM, MEM), MEM ** -0.5, 0.25)
    out_weight = scatter_about(seeds[17], (MEM, MEM), MEM ** -0.5, 0.25)
    return {"event_node": event_node, "neighbours": neighbours, "event_bucket": event_bucket, "neighbour_bucket": neighbour_bucket, "edge_features": edge_features, "affinity": affinity, "upstream": upstream, "node_memory": node_memory, "edge_weight": edge_weight, "time_message": time_message, "input_weight": input_weight, "hidden_weight": hidden_weight, "gate_bias": gate_bias, "time_key": time_key, "query_weight": query_weight, "key_weight": key_weight, "value_weight": value_weight, "out_weight": out_weight}


def make_message(edge_rows, buckets, edge_weight, time_message):
    before = jnp.dot(edge_rows, edge_weight, preferred_element_type=jnp.float32) + jnp.take(time_message, buckets, axis=0)
    return jax.nn.silu(before).astype(jnp.bfloat16)

def gru_rows(aggregate, previous, input_weight, hidden_weight, gate_bias):
    columns = previous.shape[1]
    inputs = jnp.dot(aggregate, input_weight, preferred_element_type=jnp.float32) + gate_bias
    hidden = jnp.dot(previous, hidden_weight, preferred_element_type=jnp.float32)
    update = jax.nn.sigmoid(inputs[:, :columns] + hidden[:, :columns])
    resets = jax.nn.sigmoid(inputs[:, columns:2 * columns] + hidden[:, columns:2 * columns])
    candidate = jnp.tanh(inputs[:, 2 * columns:] + resets * hidden[:, 2 * columns:])
    return (1.0 - update) * candidate + update * previous.astype(jnp.float32)

def attend(target, neighbour_rows, neighbour_bucket, affinity, time_key, query_weight, key_weight, value_weight, out_weight):
    events, fanout, columns = neighbour_rows.shape
    head_size = columns // HEADS
    query = jnp.dot(target, query_weight, preferred_element_type=jnp.float32).astype(jnp.bfloat16).reshape(events, HEADS, head_size)
    flat_rows = neighbour_rows.reshape(events * fanout, columns)
    key_rows = jnp.dot(flat_rows, key_weight, preferred_element_type=jnp.float32) + jnp.take(time_key, neighbour_bucket.reshape(-1), axis=0)
    key_rows = key_rows.astype(jnp.bfloat16).reshape(events, fanout, HEADS, head_size)
    value_rows = jnp.dot(flat_rows, value_weight, preferred_element_type=jnp.float32).astype(jnp.bfloat16).reshape(events, fanout, HEADS, head_size)
    scores = jnp.einsum('ehd,enhd->ehn', query.astype(jnp.float32), key_rows.astype(jnp.float32)) / math.sqrt(head_size)
    scores = scores + affinity[:, None, :]
    probs = jax.nn.softmax(scores, axis=-1).astype(jnp.bfloat16)
    mixed = jnp.einsum('ehn,enhd->ehd', probs.astype(jnp.float32), value_rows.astype(jnp.float32))
    mixed = mixed.astype(jnp.bfloat16).reshape(events, columns)
    return (jnp.dot(mixed, out_weight, preferred_element_type=jnp.float32) + target.astype(jnp.float32)).astype(jnp.bfloat16)

def reference(event_node, neighbours, event_bucket, neighbour_bucket, edge_features, affinity, upstream, node_memory, edge_weight, time_message, input_weight, hidden_weight, gate_bias, time_key, query_weight, key_weight, value_weight, out_weight):
    messages = make_message(edge_features, event_bucket, edge_weight, time_message)
    totals = jax.ops.segment_sum(messages.astype(jnp.float32), event_node, num_segments=NODES)
    counts = jax.ops.segment_sum(jnp.ones(event_node.shape, jnp.float32), event_node, num_segments=NODES)
    aggregate = (totals / jnp.maximum(counts, 1.0)[:, None]).astype(jnp.bfloat16)
    updated = gru_rows(aggregate, node_memory, input_weight, hidden_weight, gate_bias)
    new_memory = jnp.where(counts[:, None] > 0, updated, node_memory.astype(jnp.float32)).astype(jnp.bfloat16)

    def block(carry, number):
        start = number * EV_DEV
        targets = lax.dynamic_slice_in_dim(event_node, start, EV_DEV)
        nearby = lax.dynamic_slice_in_dim(neighbours, start, EV_DEV)
        buckets = lax.dynamic_slice_in_dim(neighbour_bucket, start, EV_DEV)
        logits = lax.dynamic_slice_in_dim(affinity, start, EV_DEV)
        tangent = lax.dynamic_slice_in_dim(upstream, start, EV_DEV)
        target_rows = jnp.take(new_memory, targets, axis=0)
        nearby_rows = jnp.take(new_memory, nearby.reshape(-1), axis=0).reshape(EV_DEV, NEIGH, MEM)

        def forward(weight_q, weight_k, weight_v, weight_o):
            return attend(target_rows, nearby_rows, buckets, logits, time_key, weight_q, weight_k, weight_v, weight_o)
        result, pullback = jax.vjp(forward, query_weight, key_weight, value_weight, out_weight)
        grads = pullback(tangent)
        carry = tuple((total + grad.astype(jnp.float32) for total, grad in zip(carry, grads)))
        return (carry, result)
    zeros_start = tuple((jnp.zeros((MEM, MEM), jnp.float32) for _ in range(4)))
    summed, blocks = lax.scan(block, zeros_start, jnp.arange(N_NODE, dtype=jnp.int32))
    embedding = blocks.reshape(EVENTS, MEM)
    factor = 1.0 / math.sqrt(EVENTS)
    return (embedding, new_memory, summed[0] * factor, summed[1] * factor, summed[2] * factor, summed[3] * factor)
```

```python
import math

import jax
import jax.numpy as jnp
from jax import lax
from jax.experimental import pallas as pl
from jax.experimental.pallas import tpu as pltpu
from jax.sharding import PartitionSpec as P

HEADS = 2
CAP = 12
SLOTS = 16
BLOCK = 64
UNROLL = 16

F32 = jnp.float32
BF16 = jnp.bfloat16


def dot(a, b):
    return jnp.dot(a, b, preferred_element_type=F32)


def dot_tn(a, b):
    return lax.dot_general(a, b, (((0,), (0,)), ((), ())), preferred_element_type=F32)


def dot_nt(a, b):
    return lax.dot_general(a, b, (((1,), (1,)), ((), ())), preferred_element_type=F32)


def flag(condition):
    return jnp.where(condition, 1.0, 0.0).astype(BF16)


def iota(shape, axis):
    return lax.broadcasted_iota(jnp.int32, shape, axis)


def sigmoid(v):
    return 1.0 / (1.0 + jnp.exp(-v))


def split_table(table):
    high = table.astype(BF16)
    low = (table - high.astype(F32)).astype(BF16)
    return jnp.concatenate([high, low], axis=0)


def pack_body(node_rows, devices, node_ref, bucket_ref, feature_ref, out_ref):
    nodes = node_ref[...]
    events = nodes.shape[1]
    owner = nodes // node_rows
    local = nodes - owner * node_rows
    marked = iota((devices, events), 0) == owner
    marks = flag(marked)
    before = flag(iota((events, events), 0) < iota((events, events), 1))
    earlier = dot(marks, before)
    rank = jnp.sum(jnp.where(marked, earlier, 0.0), axis=0, keepdims=True).astype(jnp.int32)
    lane = iota((128, events), 0)
    named = jnp.where(lane == rank, local + 1, 0) + jnp.where(
        lane == rank + SLOTS, bucket_ref[...], 0
    )
    meta = dot_nt(marks, named.astype(F32).astype(BF16)).astype(BF16)
    slots = devices * SLOTS
    place = flag(iota((slots, events), 0) == owner * SLOTS + rank)
    spots = flag(iota((slots, devices), 0) == iota((slots, devices), 1) * SLOTS + CAP)
    out_ref[...] = (dot(place, feature_ref[...]) + dot(spots, meta)).astype(BF16)


def memory_body(
    arrived_ref,
    memory_ref,
    edge_ref,
    time_ref,
    input_ref,
    hidden_ref,
    bias_ref,
    out_ref,
    rows_ref,
):
    rows_ref[...] = arrived_ref[...].astype(F32)
    sources = rows_ref.shape[0] // SLOTS
    node_rows, columns = memory_ref.shape
    previous = memory_ref[...]
    meta = rows_ref[pl.ds(CAP, sources, stride=SLOTS), :].astype(jnp.int32)
    table = split_table(time_ref[...])
    buckets = time_ref.shape[0]
    totals = jnp.zeros((node_rows, columns), F32)
    counts = jnp.zeros((node_rows, 128), F32)
    ones = jnp.ones((sources, 128), BF16)
    for r in range(CAP):
        feature = rows_ref[pl.ds(r, sources, stride=SLOTS), :].astype(BF16)
        bucket = flag(iota((sources, buckets), 1) == meta[:, SLOTS + r : SLOTS + r + 1])
        before = dot(feature, edge_ref[...]) + dot(
            jnp.concatenate([bucket, bucket], axis=1), table
        )
        message = (before / (1.0 + jnp.exp(-before))).astype(BF16)
        chosen = flag(iota((sources, node_rows), 1) + 1 == meta[:, r : r + 1])
        totals += dot_tn(chosen, message)
        counts += dot_tn(chosen, ones)
    count = counts[:, :1]
    aggregate = (totals / jnp.maximum(count, 1.0)).astype(BF16)
    inputs = dot(aggregate, input_ref[...]) + bias_ref[...]
    hidden = dot(previous, hidden_ref[...])
    update = sigmoid(inputs[:, :columns] + hidden[:, :columns])
    resets = sigmoid(inputs[:, columns : 2 * columns] + hidden[:, columns : 2 * columns])
    candidate = jnp.tanh(inputs[:, 2 * columns :] + resets * hidden[:, 2 * columns :])
    kept = previous.astype(F32)
    updated = (1.0 - update) * candidate + update * kept
    out_ref[...] = jnp.where(count > 0, updated, kept).astype(BF16)


def attend_body(
    index_ref,
    table_hbm,
    bucket_ref,
    affinity_ref,
    upstream_ref,
    time_ref,
    query_ref,
    both_ref,
    mix_ref,
    embedding_ref,
    grads_ref,
    table_ref,
    rows_ref,
    keys_ref,
    values_ref,
    change_ref,
    sums_ref,
    both_sums_ref,
    sem,
):
    step = pl.program_id(0)
    steps = pl.num_programs(0)
    block, fanout = bucket_ref.shape
    columns = query_ref.shape[0]
    head = columns // HEADS
    near = block * fanout
    picked = near + block
    pieces = columns // 128

    @pl.when(step == 0)
    def _():
        copy = pltpu.make_async_copy(table_hbm, table_ref, sem)
        copy.start()
        sums_ref[...] = jnp.zeros_like(sums_ref)
        both_sums_ref[...] = jnp.zeros_like(both_sums_ref)
        copy.wait()

    def fetch(i, carry):
        for u in range(UNROLL):
            row = i * UNROLL + u
            node = index_ref[step * picked + row]
            rows_ref[pl.ds(row * pieces, pieces), :] = table_ref[node].astype(F32)
        return carry

    lax.fori_loop(0, picked // UNROLL, fetch, 0)

    gathered = jnp.concatenate(
        [
            rows_ref[pl.ds(c, picked, stride=pieces), :].astype(BF16)
            for c in range(pieces)
        ],
        axis=1,
    )
    nearby = gathered[:near]
    target = gathered[near:]
    buckets = time_ref.shape[0] // 2
    lane = iota((block, buckets), 1)
    marks = jnp.concatenate(
        [flag(lane == bucket_ref[:, j : j + 1]) for j in range(fanout)], axis=0
    )
    keys_ref[...] = (
        dot(nearby, both_ref[:, :columns])
        + dot(jnp.concatenate([marks, marks], axis=1), time_ref[...])
    ).astype(BF16)
    values_ref[...] = dot(nearby, both_ref[:, columns:]).astype(BF16)
    query_half = dot(target, query_ref[...]).astype(BF16)
    upstream = upstream_ref[...]
    pull_half = dot_nt(upstream, mix_ref[...]).astype(BF16)
    query = query_half.astype(F32)
    pull = pull_half.astype(F32)
    scale = 1.0 / math.sqrt(head)
    mixed = []
    query_pull = []
    for h in range(HEADS):
        cols = slice(h * head, (h + 1) * head)
        q = query[:, cols]
        g = pull[:, cols]
        scores = []
        slopes = []
        for j in range(fanout):
            part = pl.ds(j * block, block)
            key = keys_ref[part, cols].astype(F32)
            value = values_ref[part, cols].astype(F32)
            score = jnp.sum(q * key, axis=1, keepdims=True) * scale
            scores.append(score + affinity_ref[:, j : j + 1])
            slope = jnp.sum(g * value, axis=1, keepdims=True)
            slopes.append(slope.astype(BF16).astype(F32))
        top = scores[0]
        for j in range(1, fanout):
            top = jnp.maximum(top, scores[j])
        powers = [jnp.exp(s - top) for s in scores]
        total = powers[0]
        for j in range(1, fanout):
            total = total + powers[j]
        over = 1.0 / total
        probs = [p * over for p in powers]
        mean = probs[0] * slopes[0]
        for j in range(1, fanout):
            mean = mean + probs[j] * slopes[j]
        mix = jnp.zeros((block, head), F32)
        back = jnp.zeros((block, head), F32)
        for j in range(fanout):
            part = pl.ds(j * block, block)
            key = keys_ref[part, cols].astype(F32)
            value = values_ref[part, cols].astype(F32)
            prob = probs[j].astype(BF16).astype(F32)
            turn = probs[j] * (slopes[j] - mean) * scale
            mix = mix + prob * value
            back = back + turn * key
            change_ref[part, cols] = (turn * q).astype(BF16)
            change_ref[part, pl.ds(columns + h * head, head)] = (prob * g).astype(BF16)
        mixed.append(mix.astype(BF16))
        query_pull.append(back.astype(BF16))
    mixed = jnp.concatenate(mixed, axis=1)
    query_pull = jnp.concatenate(query_pull, axis=1)
    embedding_ref[...] = (dot(mixed, mix_ref[...]) + target.astype(F32)).astype(BF16)
    sums_ref[:, :columns] += dot_tn(target, query_pull)
    sums_ref[:, columns:] += dot_tn(mixed, upstream)
    both_sums_ref[...] += dot_tn(nearby, change_ref[...])

    @pl.when(step == steps - 1)
    def _():
        grads_ref[pl.ds(0, columns), :] = sums_ref[:, :columns].astype(BF16)
        grads_ref[pl.ds(columns, columns), :] = both_sums_ref[:, :columns].astype(BF16)
        grads_ref[pl.ds(2 * columns, columns), :] = both_sums_ref[:, columns:].astype(BF16)
        grads_ref[pl.ds(3 * columns, columns), :] = sums_ref[:, columns:].astype(BF16)


def attend(table, index, buckets, affinity, upstream, time_pair, query_weight, both, mix_weight):
    events, fanout = buckets.shape
    columns = query_weight.shape[0]
    picked = BLOCK * (fanout + 1)
    pieces = columns // 128
    whole = lambda shape: pl.BlockSpec(shape, lambda i, *_: (0,) * len(shape))
    rows = lambda width: pl.BlockSpec((BLOCK, width), lambda i, *_: (i, 0))
    spec = pltpu.PrefetchScalarGridSpec(
        num_scalar_prefetch=1,
        grid=(events // BLOCK,),
        in_specs=[
            pl.BlockSpec(memory_space=pl.ANY),
            rows(fanout),
            rows(fanout),
            rows(columns),
            whole(time_pair.shape),
            whole(query_weight.shape),
            whole(both.shape),
            whole(mix_weight.shape),
        ],
        out_specs=[rows(columns), whole((4 * columns, columns))],
        scratch_shapes=[
            pltpu.VMEM(table.shape, BF16),
            pltpu.VMEM((picked * pieces, 128), F32),
            pltpu.VMEM((BLOCK * fanout, columns), BF16),
            pltpu.VMEM((BLOCK * fanout, columns), BF16),
            pltpu.VMEM((BLOCK * fanout, 2 * columns), BF16),
            pltpu.VMEM((columns, 2 * columns), F32),
            pltpu.VMEM((columns, 2 * columns), F32),
            pltpu.SemaphoreType.DMA,
        ],
    )
    return pl.pallas_call(
        attend_body,
        grid_spec=spec,
        out_shape=[
            jax.ShapeDtypeStruct((events, columns), BF16),
            jax.ShapeDtypeStruct((4 * columns, columns), BF16),
        ],
        compiler_params=pltpu.CompilerParams(
            dimension_semantics=("arbitrary",), vmem_limit_bytes=58 << 20
        ),
        name="attend",
    )(index, table, buckets, affinity, upstream, time_pair, query_weight, both, mix_weight)


def shards(
    event_node,
    neighbours,
    event_bucket,
    neighbour_bucket,
    edge_features,
    affinity,
    upstream,
    node_memory,
    edge_weight,
    time_message,
    input_weight,
    hidden_weight,
    gate_bias,
    time_key,
    query_weight,
    key_weight,
    value_weight,
    out_weight,
):
    devices = lax.axis_size("node")
    node_rows, columns = node_memory.shape
    events, fanout = neighbours.shape
    width = edge_features.shape[1]

    packed = pl.pallas_call(
        lambda *refs: pack_body(node_rows, devices, *refs),
        out_shape=jax.ShapeDtypeStruct((devices * SLOTS, width), BF16),
        name="pack",
    )(event_node.reshape(1, events), event_bucket.reshape(1, events), edge_features)
    arrived = lax.all_to_all(
        packed.reshape(devices, SLOTS, width), "node", split_axis=0, concat_axis=0, tiled=True
    )
    new_memory = pl.pallas_call(
        memory_body,
        out_shape=jax.ShapeDtypeStruct((node_rows, columns), BF16),
        scratch_shapes=[pltpu.VMEM((devices * SLOTS, width), F32)],
        name="memory",
    )(
        arrived.reshape(devices * SLOTS, width),
        node_memory,
        edge_weight,
        time_message,
        input_weight,
        hidden_weight,
        gate_bias.reshape(1, -1),
    )
    table = lax.all_gather(
        new_memory.reshape(node_rows, columns // 128, 128), "node", axis=0, tiled=True
    )
    steps = events // BLOCK
    index = jnp.concatenate(
        [
            neighbours.reshape(steps, BLOCK, fanout).transpose(0, 2, 1).reshape(steps, -1),
            event_node.reshape(steps, BLOCK),
        ],
        axis=1,
    ).reshape(-1)
    embedding, grads = attend(
        table,
        index,
        neighbour_bucket,
        affinity,
        upstream,
        split_table(time_key),
        query_weight,
        jnp.concatenate([key_weight, value_weight], axis=1),
        out_weight,
    )
    share = 4 * columns // devices
    parts = lax.all_to_all(
        grads.reshape(devices, share, columns), "node", split_axis=0, concat_axis=0, tiled=True
    )
    factor = 1.0 / math.sqrt(events * devices)
    own = (jnp.sum(parts.astype(F32), axis=0) * factor).astype(BF16)
    spread = lax.all_to_all(
        jnp.broadcast_to(own[None], (devices, share, columns)),
        "node",
        split_axis=0,
        concat_axis=0,
        tiled=True,
    )
    total = spread.reshape(4, columns, columns).astype(F32)
    return (embedding, new_memory, total[0], total[1], total[2], total[3])


def solution(mesh):
    placed = (
        P("node"),
        P("node", None),
        P("node"),
        P("node", None),
        P("node", None),
        P("node", None),
        P("node", None),
        P("node", None),
    ) + (P(),) * 10
    return jax.shard_map(
        shards,
        mesh=mesh,
        in_specs=placed,
        out_specs=(P("node", None), P("node", None), P(), P(), P(), P()),
        check_vma=False,
    )
```
